64 devices in a mesh: dp: 8 (over x, y, core), tp: 8 (over z).
Axes of the slice: x: 2, y: 2, z: 8, core: 2. Of those that a mesh axis runs over, the one named last changes fastest.
The devices are a block of a 4x4x8 slice.
Arguments:
- x: bfloat16 [16384, 3840], P('dp'), parts along dimension 0
- w_gate: bfloat16 [3840, 15360], P(None, 'tp')
- w_up: bfloat16 [3840, 15360], P(None, 'tp')
- w_down: bfloat16 [15360, 3840], P('tp')
Outputs:
- output: bfloat16 [16384, 3840], P('dp'), parts along dimension 0
There are 8 independent parts. The reference program is written for one: setup_inputs(seed, part) draws one part's arguments, and reference() takes and returns one part's arrays. A program takes and returns all parts, laid end to end along the dimension named above; an argument that names none is the same for every part.
All inputs are finite; a program needn't handle non-finite values.
Results may differ from the reference program's by a relative error of at most 0.016.
Values are sent between devices in bfloat16 or wider.
A program may use at most 768 MiB of HBM per device.

```python
import jax
import jax.numpy as jnp

ROWS = 2048
D = 3840
FF = 15360


def setup_inputs(seed: int = 0, part: int = 0) -> dict:
    kx, kg, ku, kd = jax.random.split(jax.random.key(seed), 4)
    drawn = {
        "x": jax.random.normal(jax.random.fold_in(kx, part), (ROWS, D), jnp.float32),
        "w_gate": jax.random.normal(kg, (D, FF), jnp.float32) * D**-0.5,
        "w_up": jax.random.normal(ku, (D, FF), jnp.float32) * D**-0.5,
        "w_down": jax.random.normal(kd, (FF, D), jnp.float32) * FF**-0.5,
    }
    return {k: v.astype(jnp.bfloat16) for k, v in drawn.items()}


def reference(x, w_gate, w_up, w_down):
    gate = jnp.dot(x, w_gate, preferred_element_type=jnp.float32)
    up = jnp.dot(x, w_up, preferred_element_type=jnp.float32)
    hidden = (jax.nn.gelu(gate) * up).astype(jnp.bfloat16)
    return jnp.dot(hidden, w_down, preferred_element_type=jnp.float32).astype(jnp.bfloat16)
```

```python
import functools

import jax
import jax.numpy as jnp
from jax import lax
from jax.experimental import pallas as pl
from jax.experimental.pallas import tpu as pltpu
from jax.sharding import PartitionSpec as P

CHUNKS = 5
AHEAD = 2
STORES = 8
VMEM_LIMIT = 67_043_328


def gated(gate, up):
    inner = 0.7978845608028654 * (gate + 0.044715 * (gate * gate * gate))
    return gate * (0.5 * (1.0 + jnp.tanh(inner))) * up


def kernel(
    n, x_ref, gate_ref, up_ref, down_ref, y_ref,
    gu_ref, wd_ref, x_buf, hid_ref,
    x_sem, gu_sem, wd_sem, send_sem, recv_sem,
):
    me = lax.axis_index("tp")
    right, left = lax.rem(me + 1, n), lax.rem(me + n - 1, n)
    peers = (right, left)
    block = x_ref.shape[0] // n
    half = block // 2
    tile = gu_ref.shape[2] // 2
    cols = wd_ref.shape[2]

    def rows_of(way, step):
        owner = lax.rem(me + 2 * n - 1 - step, n) if way == 0 else lax.rem(me + 1 + step, n)
        return pl.multiple_of(owner * block + way * half, half)

    def cols_of(k):
        return pl.ds(pl.multiple_of(k * cols, 128), cols)

    def load_x(step):
        return [
            pltpu.make_async_copy(
                x_ref.at[pl.ds(rows_of(way, step), half)],
                x_buf.at[pl.ds(way * half, half)],
                x_sem.at[way],
            )
            for way in (0, 1)
        ]

    def load_gu(j):
        at = pl.ds(pl.multiple_of(j * tile, 128), tile)
        return [
            pltpu.make_async_copy(gate_ref.at[:, at], gu_ref.at[j, :, pl.ds(0, tile)], gu_sem.at[0, j]),
            pltpu.make_async_copy(up_ref.at[:, at], gu_ref.at[j, :, pl.ds(tile, tile)], gu_sem.at[1, j]),
        ]

    def load_wd(k):
        return pltpu.make_async_copy(down_ref.at[:, cols_of(k)], wd_ref.at[k], wd_sem.at[k])

    def remote(way, step, k):
        at = y_ref.at[pl.ds(rows_of(way, step), half), cols_of(k)]
        return pltpu.make_async_remote_copy(
            src_ref=at,
            dst_ref=at,
            send_sem=send_sem.at[way, step, k],
            recv_sem=recv_sem.at[way, step, k],
            device_id={"tp": peers[way]},
            device_id_type=pl.DeviceIdType.MESH,
        )

    def arrive(way, step, k):
        at = y_ref.at[pl.ds(rows_of(way, step + 1), half), cols_of(k)]
        pltpu.make_async_remote_copy(
            src_ref=at,
            dst_ref=at,
            send_sem=send_sem.at[way, step, k],
            recv_sem=recv_sem.at[way, step, k],
            device_id={"tp": peers[way]},
            device_id_type=pl.DeviceIdType.MESH,
        ).wait_recv()

    def hidden(slot, j):
        both = jnp.dot(x_buf[...], gu_ref[j], preferred_element_type=jnp.float32)
        at = pl.ds(pl.multiple_of(j * tile, 128), tile)
        hid_ref[slot, :, at] = gated(both[:, :tile], both[:, tile:]).astype(hid_ref.dtype)

    barrier = pltpu.get_barrier_semaphore()
    for peer in peers:
        pl.semaphore_signal(barrier, inc=1, device_id={"tp": peer}, device_id_type=pl.DeviceIdType.MESH)

    def load(unit):
        @pl.when(unit < CHUNKS)
        def _():
            for copy in load_gu(unit):
                copy.start()

        @pl.when(jnp.logical_and(unit >= CHUNKS, unit < 2 * CHUNKS))
        def _():
            load_wd(unit - CHUNKS).start()

    for copy in load_x(0):
        copy.start()
    for copy in load_gu(0):
        copy.start()
    for copy in load_x(0):
        copy.wait()
    for copy in load_gu(1):
        copy.start()

    @pl.loop(0, CHUNKS)
    def _(j):
        for copy in load_gu(j):
            copy.wait()
        load(j + AHEAD)
        hidden(0, j)

    for copy in load_x(1):
        copy.start()
    pl.semaphore_wait(barrier, 2)

    @pl.loop(0, CHUNKS)
    def _(k):
        load_wd(k).wait()
        load(CHUNKS + AHEAD + k)
        term = jnp.dot(hid_ref[0], wd_ref[k], preferred_element_type=jnp.float32)
        for way in (0, 1):
            at = (pl.ds(rows_of(way, 0), half), cols_of(k))
            y_ref[at] = term[way * half : (way + 1) * half].astype(y_ref.dtype)
            remote(way, 0, k).start()

    for copy in load_x(1):
        copy.wait()

    @pl.loop(0, CHUNKS)
    def _(j):
        hidden(1, j)

    @pl.loop(1, n)
    def _(step):
        slot = lax.rem(step, 2)
        more = step < n - 1

        @pl.when(more)
        def _():
            for copy in load_x(step + 1):
                copy.start()

        @pl.loop(0, CHUNKS)
        def _(k):
            term = jnp.dot(hid_ref[slot], wd_ref[k], preferred_element_type=jnp.float32)
            for way in (0, 1):
                arrive(way, step - 1, k)

            @pl.when(step > 1)
            def _():
                for way in (0, 1):
                    remote(way, step - 2, k).wait_send()

            for way in (0, 1):
                at = (pl.ds(rows_of(way, step), half), cols_of(k))
                total = y_ref[at].astype(jnp.float32) + term[way * half : (way + 1) * half]
                y_ref[at] = total.astype(y_ref.dtype)
                remote(way, step, k).start()

            @pl.when(jnp.logical_and(more, k == 0))
            def _():
                for copy in load_x(step + 1):
                    copy.wait()

            @pl.when(more)
            def _():
                hidden(1 - slot, k)

    @pl.loop(n, 2 * n - 2)
    def _(step):
        @pl.loop(0, CHUNKS)
        def _(k):
            for way in (0, 1):
                arrive(way, step - 1, k)
                remote(way, step - 2, k).wait_send()
                remote(way, step, k).start()

    @pl.loop(0, CHUNKS)
    def _(k):
        for way in (0, 1):
            arrive(way, 2 * n - 3, k)

    @pl.loop(2 * n - 4, 2 * n - 2)
    def _(step):
        @pl.loop(0, CHUNKS)
        def _(k):
            for way in (0, 1):
                remote(way, step, k).wait_send()


def store(y_ref, out_ref, sem):
    rows = y_ref.shape[0] // STORES
    copies = [
        pltpu.make_async_copy(y_ref.at[pl.ds(i * rows, rows)], out_ref.at[pl.ds(i * rows, rows)], sem.at[i])
        for i in range(STORES)
    ]
    for copy in copies:
        copy.start()
    for copy in copies:
        copy.wait()


def solution(mesh):
    n = mesh.shape["tp"]
    hops = 2 * n - 2

    def step(x, w_gate, w_up, w_down):
        rows, width = x.shape
        units = w_gate.shape[1]
        block = rows // n
        y = pl.pallas_call(
            functools.partial(kernel, n),
            out_shape=pltpu.VMEM((rows, width), jnp.bfloat16),
            in_specs=[pl.BlockSpec(memory_space=pl.ANY)] * 4,
            out_specs=pl.BlockSpec(memory_space=pltpu.VMEM),
            scratch_shapes=[
                pltpu.VMEM((CHUNKS, width, 2 * units // CHUNKS), jnp.bfloat16),
                pltpu.VMEM((CHUNKS, units, width // CHUNKS), jnp.bfloat16),
                pltpu.VMEM((block, width), jnp.bfloat16),
                pltpu.VMEM((2, block, units), jnp.bfloat16),
                pltpu.SemaphoreType.DMA((2,)),
                pltpu.SemaphoreType.DMA((2, CHUNKS)),
                pltpu.SemaphoreType.DMA((CHUNKS,)),
                pltpu.SemaphoreType.DMA((2, hops, CHUNKS)),
                pltpu.SemaphoreType.DMA((2, hops, CHUNKS)),
            ],
            compiler_params=pltpu.CompilerParams(
                collective_id=0,
                has_side_effects=True,
                vmem_limit_bytes=VMEM_LIMIT - rows * width * 2,
            ),
        )(x, w_gate, w_up, w_down)
        return pl.pallas_call(
            store,
            out_shape=jax.ShapeDtypeStruct((rows, width), jnp.bfloat16),
            in_specs=[pl.BlockSpec(memory_space=pl.ANY)],
            out_specs=pl.BlockSpec(memory_space=pl.ANY),
            scratch_shapes=[pltpu.SemaphoreType.DMA((STORES,))],
            compiler_params=pltpu.CompilerParams(vmem_limit_bytes=1 << 20),
        )(pltpu.with_memory_space_constraint(y, pltpu.VMEM))

    return jax.shard_map(
        step,
        mesh=mesh,
        in_specs=(P("dp", None), P(None, "tp"), P(None, "tp"), P("tp", None)),
        out_specs=P("dp", None),
        check_vma=False,
    )
```

```python
import functools

import jax
import jax.numpy as jnp
from jax import lax
from jax.experimental import pallas as pl
from jax.experimental.pallas import tpu as pltpu
from jax.sharding import PartitionSpec as P

CHUNKS = 5
AHEAD = 2
STORES = 8
VMEM_LIMIT = 67_043_328


def gated(gate, up):
    inner = 0.7978845608028654 * (gate + 0.044715 * (gate * gate * gate))
    return gate * (0.5 * (1.0 + jnp.tanh(inner))) * up


def rows_of(n, block, me, way, step):
    owner = lax.rem(me + 2 * n - 1 - step, n) if way == 0 else lax.rem(me + 1 + step, n)
    return pl.multiple_of(owner * block + way * (block // 2), block // 2)


def split(n):
    return 2 * n - 4 + lax.rem(lax.axis_index("dp"), 2)


def kernel(
    n, x_ref, gate_ref, up_ref, down_ref, y_ref,
    gu_ref, wd_ref, x_buf, hid_ref,
    x_sem, gu_sem, wd_sem, send_sem, recv_sem,
):
    me = lax.axis_index("tp")
    right, left = lax.rem(me + 1, n), lax.rem(me + n - 1, n)
    peers = (right, left)
    block = x_ref.shape[0] // n
    half = block // 2
    tile = gu_ref.shape[2] // 2
    cols = wd_ref.shape[2]

    def cols_of(k):
        return pl.ds(pl.multiple_of(k * cols, 128), cols)

    def load_x(step):
        return [
            pltpu.make_async_copy(
                x_ref.at[pl.ds(rows_of(n, block, me, way, step), half)],
                x_buf.at[pl.ds(way * half, half)],
                x_sem.at[way],
            )
            for way in (0, 1)
        ]

    def load_gu(j):
        at = pl.ds(pl.multiple_of(j * tile, 128), tile)
        return [
            pltpu.make_async_copy(gate_ref.at[:, at], gu_ref.at[j, :, pl.ds(0, tile)], gu_sem.at[0, j]),
            pltpu.make_async_copy(up_ref.at[:, at], gu_ref.at[j, :, pl.ds(tile, tile)], gu_sem.at[1, j]),
        ]

    def load_wd(k):
        return pltpu.make_async_copy(down_ref.at[:, cols_of(k)], wd_ref.at[k], wd_sem.at[k])

    def remote(way, step, k):
        at = y_ref.at[pl.ds(rows_of(n, block, me, way, step), half), cols_of(k)]
        return pltpu.make_async_remote_copy(
            src_ref=at,
            dst_ref=at,
            send_sem=send_sem.at[way, step, k],
            recv_sem=recv_sem.at[way, step, k],
            device_id={"tp": peers[way]},
            device_id_type=pl.DeviceIdType.MESH,
        )

    def arrive(way, step, k):
        at = y_ref.at[pl.ds(rows_of(n, block, me, way, step + 1), half), cols_of(k)]
        pltpu.make_async_remote_copy(
            src_ref=at,
            dst_ref=at,
            send_sem=send_sem.at[way, step, k],
            recv_sem=recv_sem.at[way, step, k],
            device_id={"tp": peers[way]},
            device_id_type=pl.DeviceIdType.MESH,
        ).wait_recv()

    def hidden(slot, j):
        both = jnp.dot(x_buf[...], gu_ref[j], preferred_element_type=jnp.float32)
        at = pl.ds(pl.multiple_of(j * tile, 128), tile)
        hid_ref[slot, :, at] = gated(both[:, :tile], both[:, tile:]).astype(hid_ref.dtype)

    barrier = pltpu.get_barrier_semaphore()
    for peer in peers:
        pl.semaphore_signal(barrier, inc=1, device_id={"tp": peer}, device_id_type=pl.DeviceIdType.MESH)

    def load(unit):
        @pl.when(unit < CHUNKS)
        def _():
            for copy in load_gu(unit):
                copy.start()

        @pl.when(jnp.logical_and(unit >= CHUNKS, unit < 2 * CHUNKS))
        def _():
            load_wd(unit - CHUNKS).start()

    for copy in load_x(0):
        copy.start()
    for copy in load_gu(0):
        copy.start()
    for copy in load_x(0):
        copy.wait()
    for copy in load_gu(1):
        copy.start()

    @pl.loop(0, CHUNKS)
    def _(j):
        for copy in load_gu(j):
            copy.wait()
        load(j + AHEAD)
        hidden(0, j)

    for copy in load_x(1):
        copy.start()
    pl.semaphore_wait(barrier, 2)

    @pl.loop(0, CHUNKS)
    def _(k):
        load_wd(k).wait()
        load(CHUNKS + AHEAD + k)
        term = jnp.dot(hid_ref[0], wd_ref[k], preferred_element_type=jnp.float32)
        for way in (0, 1):
            at = (pl.ds(rows_of(n, block, me, way, 0), half), cols_of(k))
            y_ref[at] = term[way * half : (way + 1) * half].astype(y_ref.dtype)
            remote(way, 0, k).start()

    for copy in load_x(1):
        copy.wait()

    @pl.loop(0, CHUNKS)
    def _(j):
        hidden(1, j)

    @pl.loop(1, n)
    def _(step):
        slot = lax.rem(step, 2)
        more = step < n - 1

        @pl.when(more)
        def _():
            for copy in load_x(step + 1):
                copy.start()

        @pl.loop(0, CHUNKS)
        def _(k):
            term = jnp.dot(hid_ref[slot], wd_ref[k], preferred_element_type=jnp.float32)
            for way in (0, 1):
                arrive(way, step - 1, k)

            @pl.when(step > 1)
            def _():
                for way in (0, 1):
                    remote(way, step - 2, k).wait_send()

            for way in (0, 1):
                at = (pl.ds(rows_of(n, block, me, way, step), half), cols_of(k))
                total = y_ref[at].astype(jnp.float32) + term[way * half : (way + 1) * half]
                y_ref[at] = total.astype(y_ref.dtype)
                remote(way, step, k).start()

            @pl.when(jnp.logical_and(more, k == 0))
            def _():
                for copy in load_x(step + 1):
                    copy.wait()

            @pl.when(more)
            def _():
                hidden(1 - slot, k)

    last = split(n)

    @pl.loop(n, last)
    def _(step):
        @pl.loop(0, CHUNKS)
        def _(k):
            for way in (0, 1):
                arrive(way, step - 1, k)
                remote(way, step - 2, k).wait_send()
                remote(way, step, k).start()

    @pl.loop(0, CHUNKS)
    def _(k):
        for way in (0, 1):
            arrive(way, last - 1, k)

    @pl.loop(last - 2, last)
    def _(step):
        @pl.loop(0, CHUNKS)
        def _(k):
            for way in (0, 1):
                remote(way, step, k).wait_send()


def finish(n, y_ref, early_ref, late_ref, send_sem, recv_sem):
    del early_ref
    me = lax.axis_index("tp")
    peers = (lax.rem(me + 1, n), lax.rem(me + n - 1, n))
    block = y_ref.shape[0] // n
    half = block // 2
    cols = y_ref.shape[1] // CHUNKS
    two = split(n) == 2 * n - 4

    barrier = pltpu.get_barrier_semaphore()
    for peer in peers:
        pl.semaphore_signal(barrier, inc=1, device_id={"tp": peer}, device_id_type=pl.DeviceIdType.MESH)
    pl.semaphore_wait(barrier, 2)

    def remote(way, i, k, stored):
        at = pl.ds(pl.multiple_of(k * cols, 128), cols)
        rows = pl.ds(rows_of(n, block, me, way, 2 * n - 4 + i), half)
        return pltpu.make_async_remote_copy(
            src_ref=late_ref.at[way, 0, :, at] if stored else y_ref.at[rows, at],
            dst_ref=late_ref.at[way, i, :, at],
            send_sem=send_sem.at[way, i, k],
            recv_sem=recv_sem.at[way, i, k],
            device_id={"tp": peers[way]},
            device_id_type=pl.DeviceIdType.MESH,
        )

    @pl.when(two)
    def _():
        @pl.loop(0, CHUNKS)
        def _(k):
            for way in (0, 1):
                remote(way, 0, k, False).start()

        @pl.loop(0, CHUNKS)
        def _(k):
            for way in (0, 1):
                remote(way, 0, k, False).wait_recv()
                remote(way, 1, k, True).start()

        @pl.loop(0, CHUNKS)
        def _(k):
            for way in (0, 1):
                remote(way, 0, k, False).wait_send()

    @pl.when(jnp.logical_not(two))
    def _():
        @pl.loop(0, CHUNKS)
        def _(k):
            for way in (0, 1):
                remote(way, 1, k, False).start()

    @pl.loop(0, CHUNKS)
    def _(k):
        for way in (0, 1):
            remote(way, 1, k, True).wait()


def store(y_ref, out_ref, sem):
    rows = y_ref.shape[0] // STORES
    copies = [
        pltpu.make_async_copy(y_ref.at[pl.ds(i * rows, rows)], out_ref.at[pl.ds(i * rows, rows)], sem.at[i])
        for i in range(STORES)
    ]
    for copy in copies:
        copy.start()
    for copy in copies:
        copy.wait()


def store_late(n, early_ref, late_ref, out_ref, sem):
    del early_ref
    me = lax.axis_index("tp")
    block = out_ref.shape[0] // n

    def copy(way, i):
        rows = pl.ds(rows_of(n, block, me, way, 2 * n - 3 + i), block // 2)
        return pltpu.make_async_copy(late_ref.at[way, i], out_ref.at[rows], sem.at[way, i])

    two = split(n) == 2 * n - 4

    @pl.when(two)
    def _():
        for way in (0, 1):
            copy(way, 0).start()

    for way in (0, 1):
        copy(way, 1).start()
    for way in (0, 1):
        copy(way, 1).wait()

    @pl.when(two)
    def _():
        for way in (0, 1):
            copy(way, 0).wait()


def solution(mesh):
    n = mesh.shape["tp"]
    hops = 2 * n - 2

    def step(x, w_gate, w_up, w_down):
        rows, width = x.shape
        units = w_gate.shape[1]
        block = rows // n
        y = pl.pallas_call(
            functools.partial(kernel, n),
            out_shape=pltpu.VMEM((rows, width), jnp.bfloat16),
            in_specs=[pl.BlockSpec(memory_space=pl.ANY)] * 4,
            out_specs=pl.BlockSpec(memory_space=pltpu.VMEM),
            scratch_shapes=[
                pltpu.VMEM((CHUNKS, width, 2 * units // CHUNKS), jnp.bfloat16),
                pltpu.VMEM((CHUNKS, units, width // CHUNKS), jnp.bfloat16),
                pltpu.VMEM((block, width), jnp.bfloat16),
                pltpu.VMEM((2, block, units), jnp.bfloat16),
                pltpu.SemaphoreType.DMA((2,)),
                pltpu.SemaphoreType.DMA((2, CHUNKS)),
                pltpu.SemaphoreType.DMA((CHUNKS,)),
                pltpu.SemaphoreType.DMA((2, hops, CHUNKS)),
                pltpu.SemaphoreType.DMA((2, hops, CHUNKS)),
            ],
            compiler_params=pltpu.CompilerParams(
                collective_id=0,
                has_side_effects=True,
                vmem_limit_bytes=VMEM_LIMIT - rows * width * 2,
            ),
        )(x, w_gate, w_up, w_down)
        y = pltpu.with_memory_space_constraint(y, pltpu.VMEM)
        anywhere = pl.BlockSpec(memory_space=pl.ANY)
        early = pl.pallas_call(
            store,
            out_shape=jax.ShapeDtypeStruct((rows, width), jnp.bfloat16),
            in_specs=[anywhere],
            out_specs=anywhere,
            scratch_shapes=[pltpu.SemaphoreType.DMA((STORES,))],
            compiler_params=pltpu.CompilerParams(vmem_limit_bytes=1 << 20),
        )(y)
        late = pl.pallas_call(
            functools.partial(finish, n),
            out_shape=pltpu.VMEM((2, 2, block // 2, width), jnp.bfloat16),
            in_specs=[anywhere] * 2,
            out_specs=anywhere,
            scratch_shapes=[
                pltpu.SemaphoreType.DMA((2, 2, CHUNKS)),
                pltpu.SemaphoreType.DMA((2, 2, CHUNKS)),
            ],
            compiler_params=pltpu.CompilerParams(
                collective_id=1, has_side_effects=True, vmem_limit_bytes=1 << 20
            ),
        )(y, pltpu.with_memory_space_constraint(early, pltpu.HBM))
        late = pltpu.with_memory_space_constraint(late, pltpu.VMEM)
        return pl.pallas_call(
            functools.partial(store_late, n),
            out_shape=jax.ShapeDtypeStruct((rows, width), jnp.bfloat16),
            in_specs=[anywhere] * 2,
            out_specs=anywhere,
            input_output_aliases={0: 0},
            scratch_shapes=[pltpu.SemaphoreType.DMA((2, 2))],
            compiler_params=pltpu.CompilerParams(vmem_limit_bytes=1 << 20),
        )(early, late)

    return jax.shard_map(
        step,
        mesh=mesh,
        in_specs=(P("dp", None), P(None, "tp"), P(None, "tp"), P("tp", None)),
        out_specs=P("dp", None),
        check_vma=False,
    )
```

```python
import functools

import jax
import jax.numpy as jnp
from jax import lax
from jax.experimental import pallas as pl
from jax.experimental.pallas import tpu as pltpu
from jax.sharding import PartitionSpec as P

CHUNKS = 5
AHEAD = 2
STORES = 16
VMEM_LIMIT = 67_043_328
LEFT = (10, 3)


def gated(gate, up):
    inner = 0.7978845608028654 * (gate + 0.044715 * (gate * gate * gate))
    return gate * (0.5 * (1.0 + jnp.tanh(inner))) * up


def rows_of(n, block, me, way, step):
    owner = lax.rem(me + 2 * n - 1 - step, n) if way == 0 else lax.rem(me + 1 + step, n)
    return pl.multiple_of(owner * block + way * (block // 2), block // 2)


def split(n):
    total = (2 * n - 2) * CHUNKS
    return total - LEFT[0] + (LEFT[0] - LEFT[1]) * lax.rem(lax.axis_index("dp"), 2), total


def kernel(
    n, x_ref, gate_ref, up_ref, down_ref, y_ref,
    gu_ref, wd_ref, x_buf, hid_ref,
    x_sem, gu_sem, wd_sem, send_sem, recv_sem,
):
    me = lax.axis_index("tp")
    right, left = lax.rem(me + 1, n), lax.rem(me + n - 1, n)
    peers = (right, left)
    block = x_ref.shape[0] // n
    half = block // 2
    tile = gu_ref.shape[2] // 2
    cols = wd_ref.shape[2]

    def cols_of(k):
        return pl.ds(pl.multiple_of(k * cols, 128), cols)

    def load_x(step):
        return [
            pltpu.make_async_copy(
                x_ref.at[pl.ds(rows_of(n, block, me, way, step), half)],
                x_buf.at[pl.ds(way * half, half)],
                x_sem.at[way],
            )
            for way in (0, 1)
        ]

    def load_gu(j):
        at = pl.ds(pl.multiple_of(j * tile, 128), tile)
        return [
            pltpu.make_async_copy(gate_ref.at[:, at], gu_ref.at[j, :, pl.ds(0, tile)], gu_sem.at[0, j]),
            pltpu.make_async_copy(up_ref.at[:, at], gu_ref.at[j, :, pl.ds(tile, tile)], gu_sem.at[1, j]),
        ]

    def load_wd(k):
        return pltpu.make_async_copy(down_ref.at[:, cols_of(k)], wd_ref.at[k], wd_sem.at[k])

    def remote(way, step, k):
        at = y_ref.at[pl.ds(rows_of(n, block, me, way, step), half), cols_of(k)]
        return pltpu.make_async_remote_copy(
            src_ref=at,
            dst_ref=at,
            send_sem=send_sem.at[way, step, k],
            recv_sem=recv_sem.at[way, step, k],
            device_id={"tp": peers[way]},
            device_id_type=pl.DeviceIdType.MESH,
        )

    def arrive(way, step, k):
        at = y_ref.at[pl.ds(rows_of(n, block, me, way, step + 1), half), cols_of(k)]
        pltpu.make_async_remote_copy(
            src_ref=at,
            dst_ref=at,
            send_sem=send_sem.at[way, step, k],
            recv_sem=recv_sem.at[way, step, k],
            device_id={"tp": peers[way]},
            device_id_type=pl.DeviceIdType.MESH,
        ).wait_recv()

    def hidden(slot, j):
        both = jnp.dot(x_buf[...], gu_ref[j], preferred_element_type=jnp.float32)
        at = pl.ds(pl.multiple_of(j * tile, 128), tile)
        hid_ref[slot, :, at] = gated(both[:, :tile], both[:, tile:]).astype(hid_ref.dtype)

    barrier = pltpu.get_barrier_semaphore()
    for peer in peers:
        pl.semaphore_signal(barrier, inc=1, device_id={"tp": peer}, device_id_type=pl.DeviceIdType.MESH)

    def load(unit):
        @pl.when(unit < CHUNKS)
        def _():
            for copy in load_gu(unit):
                copy.start()

        @pl.when(jnp.logical_and(unit >= CHUNKS, unit < 2 * CHUNKS))
        def _():
            load_wd(unit - CHUNKS).start()

    for copy in load_x(0):
        copy.start()
    for copy in load_gu(0):
        copy.start()
    for copy in load_x(0):
        copy.wait()
    for copy in load_gu(1):
        copy.start()

    @pl.loop(0, CHUNKS)
    def _(j):
        for copy in load_gu(j):
            copy.wait()
        load(j + AHEAD)
        hidden(0, j)

    for copy in load_x(1):
        copy.start()
    pl.semaphore_wait(barrier, 2)

    @pl.loop(0, CHUNKS)
    def _(k):
        load_wd(k).wait()
        load(CHUNKS + AHEAD + k)
        term = jnp.dot(hid_ref[0], wd_ref[k], preferred_element_type=jnp.float32)
        for way in (0, 1):
            at = (pl.ds(rows_of(n, block, me, way, 0), half), cols_of(k))
            y_ref[at] = term[way * half : (way + 1) * half].astype(y_ref.dtype)
            remote(way, 0, k).start()

    for copy in load_x(1):
        copy.wait()

    @pl.loop(0, CHUNKS)
    def _(j):
        hidden(1, j)

    @pl.loop(1, n)
    def _(step):
        slot = lax.rem(step, 2)
        more = step < n - 1

        @pl.when(more)
        def _():
            for copy in load_x(step + 1):
                copy.start()

        @pl.loop(0, CHUNKS)
        def _(k):
            term = jnp.dot(hid_ref[slot], wd_ref[k], preferred_element_type=jnp.float32)
            for way in (0, 1):
                arrive(way, step - 1, k)

            @pl.when(step > 1)
            def _():
                for way in (0, 1):
                    remote(way, step - 2, k).wait_send()

            for way in (0, 1):
                at = (pl.ds(rows_of(n, block, me, way, step), half), cols_of(k))
                total = y_ref[at].astype(jnp.float32) + term[way * half : (way + 1) * half]
                y_ref[at] = total.astype(y_ref.dtype)
                remote(way, step, k).start()

            @pl.when(jnp.logical_and(more, k == 0))
            def _():
                for copy in load_x(step + 1):
                    copy.wait()

            @pl.when(more)
            def _():
                hidden(1 - slot, k)

    cut, _ = split(n)

    @pl.loop(n * CHUNKS, cut)
    def _(i):
        step, k = i // CHUNKS, lax.rem(i, CHUNKS)
        for way in (0, 1):
            arrive(way, step - 1, k)
            remote(way, step - 2, k).wait_send()
            remote(way, step, k).start()

    @pl.loop(cut - CHUNKS, cut)
    def _(i):
        for way in (0, 1):
            arrive(way, i // CHUNKS, lax.rem(i, CHUNKS))

    @pl.loop(cut - 2 * CHUNKS, cut)
    def _(i):
        for way in (0, 1):
            remote(way, i // CHUNKS, lax.rem(i, CHUNKS)).wait_send()


def finish(n, y_ref, early_ref, late_ref, send_sem, recv_sem):
    del early_ref
    me = lax.axis_index("tp")
    peers = (lax.rem(me + 1, n), lax.rem(me + n - 1, n))
    block = y_ref.shape[0] // n
    half = block // 2
    cols = y_ref.shape[1] // CHUNKS
    cut, total = split(n)

    barrier = pltpu.get_barrier_semaphore()
    for peer in peers:
        pl.semaphore_signal(barrier, inc=1, device_id={"tp": peer}, device_id_type=pl.DeviceIdType.MESH)
    pl.semaphore_wait(barrier, 2)

    def remote(way, i, stored):
        at = pl.ds(pl.multiple_of(lax.rem(i, CHUNKS) * cols, 128), cols)
        rows = pl.ds(rows_of(n, block, me, way, i // CHUNKS), half)
        return pltpu.make_async_remote_copy(
            src_ref=late_ref.at[way, i - CHUNKS - cut] if stored else y_ref.at[rows, at],
            dst_ref=late_ref.at[way, i - cut],
            send_sem=send_sem.at[way, i - cut],
            recv_sem=recv_sem.at[way, i - cut],
            device_id={"tp": peers[way]},
            device_id_type=pl.DeviceIdType.MESH,
        )

    middle = jnp.minimum(cut + CHUNKS, total)

    @pl.loop(cut, middle)
    def _(i):
        for way in (0, 1):
            remote(way, i, False).start()

    @pl.loop(middle, total)
    def _(i):
        for way in (0, 1):
            remote(way, i - CHUNKS, False).wait_recv()
            remote(way, i, True).start()

    @pl.loop(jnp.maximum(cut, total - CHUNKS), total)
    def _(i):
        for way in (0, 1):
            remote(way, i, False).wait_recv()

    @pl.loop(cut, total)
    def _(i):
        for way in (0, 1):
            remote(way, i, False).wait_send()


def store(y_ref, out_ref, sem):
    rows = y_ref.shape[0] // STORES
    copies = [
        pltpu.make_async_copy(y_ref.at[pl.ds(i * rows, rows)], out_ref.at[pl.ds(i * rows, rows)], sem.at[i])
        for i in range(STORES)
    ]
    for copy in copies:
        copy.start()
    for copy in copies:
        copy.wait()


def store_late(n, early_ref, late_ref, out_ref, sem):
    del early_ref
    me = lax.axis_index("tp")
    block = out_ref.shape[0] // n
    cols = out_ref.shape[1] // CHUNKS
    cut, total = split(n)

    def copy(way, i):
        at = pl.ds(pl.multiple_of(lax.rem(i, CHUNKS) * cols, 128), cols)
        rows = pl.ds(rows_of(n, block, me, way, i // CHUNKS + 1), block // 2)
        return pltpu.make_async_copy(late_ref.at[way, i - cut], out_ref.at[rows, at], sem.at[way, i - cut])

    @pl.loop(cut, total)
    def _(i):
        for way in (0, 1):
            copy(way, i).start()

    @pl.loop(cut, total)
    def _(i):
        for way in (0, 1):
            copy(way, i).wait()


def solution(mesh):
    n = mesh.shape["tp"]
    hops = 2 * n - 2

    def step(x, w_gate, w_up, w_down):
        rows, width = x.shape
        units = w_gate.shape[1]
        block = rows // n
        y = pl.pallas_call(
            functools.partial(kernel, n),
            out_shape=pltpu.VMEM((rows, width), jnp.bfloat16),
            in_specs=[pl.BlockSpec(memory_space=pl.ANY)] * 4,
            out_specs=pl.BlockSpec(memory_space=pltpu.VMEM),
            scratch_shapes=[
                pltpu.VMEM((CHUNKS, width, 2 * units // CHUNKS), jnp.bfloat16),
                pltpu.VMEM((CHUNKS, units, width // CHUNKS), jnp.bfloat16),
                pltpu.VMEM((block, width), jnp.bfloat16),
                pltpu.VMEM((2, block, units), jnp.bfloat16),
                pltpu.SemaphoreType.DMA((2,)),
                pltpu.SemaphoreType.DMA((2, CHUNKS)),
                pltpu.SemaphoreType.DMA((CHUNKS,)),
                pltpu.SemaphoreType.DMA((2, hops, CHUNKS)),
                pltpu.SemaphoreType.DMA((2, hops, CHUNKS)),
            ],
            compiler_params=pltpu.CompilerParams(
                collective_id=0,
                has_side_effects=True,
                vmem_limit_bytes=VMEM_LIMIT - rows * width * 2,
            ),
        )(x, w_gate, w_up, w_down)
        y = pltpu.with_memory_space_constraint(y, pltpu.VMEM)
        anywhere = pl.BlockSpec(memory_space=pl.ANY)
        early = pl.pallas_call(
            store,
            out_shape=jax.ShapeDtypeStruct((rows, width), jnp.bfloat16),
            in_specs=[anywhere],
            out_specs=anywhere,
            scratch_shapes=[pltpu.SemaphoreType.DMA((STORES,))],
            compiler_params=pltpu.CompilerParams(vmem_limit_bytes=1 << 20),
        )(y)
        late = pl.pallas_call(
            functools.partial(finish, n),
            out_shape=pltpu.VMEM((2, LEFT[0], block // 2, width // CHUNKS), jnp.bfloat16),
            in_specs=[anywhere] * 2,
            out_specs=anywhere,
            scratch_shapes=[
                pltpu.SemaphoreType.DMA((2, LEFT[0])),
                pltpu.SemaphoreType.DMA((2, LEFT[0])),
            ],
            compiler_params=pltpu.CompilerParams(
                collective_id=1, has_side_effects=True, vmem_limit_bytes=1 << 20
            ),
        )(y, pltpu.with_memory_space_constraint(early, pltpu.HBM))
        late = pltpu.with_memory_space_constraint(late, pltpu.VMEM)
        return pl.pallas_call(
            functools.partial(store_late, n),
            out_shape=jax.ShapeDtypeStruct((rows, width), jnp.bfloat16),
            in_specs=[anywhere] * 2,
            out_specs=anywhere,
            input_output_aliases={0: 0},
            scratch_shapes=[pltpu.SemaphoreType.DMA((2, LEFT[0]))],
            compiler_params=pltpu.CompilerParams(vmem_limit_bytes=1 << 20),
        )(early, late)

    return jax.shard_map(
        step,
        mesh=mesh,
        in_specs=(P("dp", None), P(None, "tp"), P(None, "tp"), P("tp", None)),
        out_specs=P("dp", None),
        check_vma=False,
    )
```

```python
import functools

import jax
import jax.numpy as jnp
from jax import lax
from jax.experimental import pallas as pl
from jax.experimental.pallas import tpu as pltpu
from jax.sharding import PartitionSpec as P

CHUNKS = 5
AHEAD = 2
PART = 256
STORES = 16
VMEM_LIMIT = 67_043_328
LEFT = (9, 2)


def gated(gate, up):
    inner = 0.7978845608028654 * (gate + 0.044715 * (gate * gate * gate))
    return gate * (0.5 * (1.0 + jnp.tanh(inner))) * up


def rows_of(n, block, me, way, step):
    owner = lax.rem(me + 2 * n - 1 - step, n) if way == 0 else lax.rem(me + 1 + step, n)
    return pl.multiple_of(owner * block + way * (block // 2), block // 2)


def split(n):
    total = (2 * n - 2) * CHUNKS
    return total - LEFT[0] + (LEFT[0] - LEFT[1]) * lax.rem(lax.axis_index("dp"), 2), total


def kernel(
    n, x_ref, gate_ref, up_ref, down_ref, y_ref,
    gu_ref, wd_ref, x_buf, hid_ref,
    x_sem, gu_sem, wd_sem, send_sem, recv_sem,
):
    me = lax.axis_index("tp")
    right, left = lax.rem(me + 1, n), lax.rem(me + n - 1, n)
    peers = (right, left)
    block = x_ref.shape[0] // n
    half = block // 2
    tile = gu_ref.shape[2] // 2
    cols = wd_ref.shape[2]

    def cols_of(k):
        return pl.ds(pl.multiple_of(k * cols, 128), cols)

    def load_x(step):
        return [
            pltpu.make_async_copy(
                x_ref.at[pl.ds(rows_of(n, block, me, way, step), half)],
                x_buf.at[pl.ds(way * half, half)],
                x_sem.at[way],
            )
            for way in (0, 1)
        ]

    def load_gu(j):
        at = pl.ds(pl.multiple_of(j * tile, 128), tile)
        return [
            pltpu.make_async_copy(gate_ref.at[:, at], gu_ref.at[j, :, pl.ds(0, tile)], gu_sem.at[0, j]),
            pltpu.make_async_copy(up_ref.at[:, at], gu_ref.at[j, :, pl.ds(tile, tile)], gu_sem.at[1, j]),
        ]

    def load_wd(k):
        return pltpu.make_async_copy(down_ref.at[:, cols_of(k)], wd_ref.at[k], wd_sem.at[k])

    def remote(way, step, k):
        at = y_ref.at[pl.ds(rows_of(n, block, me, way, step), half), cols_of(k)]
        return pltpu.make_async_remote_copy(
            src_ref=at,
            dst_ref=at,
            send_sem=send_sem.at[way, step, k],
            recv_sem=recv_sem.at[way, step, k],
            device_id={"tp": peers[way]},
            device_id_type=pl.DeviceIdType.MESH,
        )

    def arrive(way, step, k):
        at = y_ref.at[pl.ds(rows_of(n, block, me, way, step + 1), half), cols_of(k)]
        pltpu.make_async_remote_copy(
            src_ref=at,
            dst_ref=at,
            send_sem=send_sem.at[way, step, k],
            recv_sem=recv_sem.at[way, step, k],
            device_id={"tp": peers[way]},
            device_id_type=pl.DeviceIdType.MESH,
        ).wait_recv()

    def hidden(slot, j):
        both = jnp.dot(x_buf[...], gu_ref[j], preferred_element_type=jnp.float32)
        at = pl.ds(pl.multiple_of(j * tile, 128), tile)
        hid_ref[slot, :, at] = gated(both[:, :tile], both[:, tile:]).astype(hid_ref.dtype)

    barrier = pltpu.get_barrier_semaphore()
    for peer in peers:
        pl.semaphore_signal(barrier, inc=1, device_id={"tp": peer}, device_id_type=pl.DeviceIdType.MESH)

    def load(unit):
        @pl.when(unit < CHUNKS)
        def _():
            for copy in load_gu(unit):
                copy.start()

        @pl.when(jnp.logical_and(unit >= CHUNKS, unit < 2 * CHUNKS))
        def _():
            load_wd(unit - CHUNKS).start()

    for copy in load_x(0):
        copy.start()
    for copy in load_gu(0):
        copy.start()
    for copy in load_x(0):
        copy.wait()
    for copy in load_gu(1):
        copy.start()

    @pl.loop(0, CHUNKS)
    def _(j):
        for copy in load_gu(j):
            copy.wait()
        load(j + AHEAD)
        hidden(0, j)

    for copy in load_x(1):
        copy.start()
    pl.semaphore_wait(barrier, 2)

    load_wd(0).wait()
    load(CHUNKS + AHEAD)
    for part in range(cols // PART):
        term = jnp.dot(hid_ref[0], wd_ref[0, :, part * PART : (part + 1) * PART], preferred_element_type=jnp.float32)
        for way in (0, 1):
            at = (pl.ds(rows_of(n, block, me, way, 0), half), pl.ds(part * PART, PART))
            y_ref[at] = term[way * half : (way + 1) * half].astype(y_ref.dtype)
            pltpu.make_async_remote_copy(
                src_ref=y_ref.at[at],
                dst_ref=y_ref.at[at],
                send_sem=send_sem.at[way, 0, 0],
                recv_sem=recv_sem.at[way, 0, 0],
                device_id={"tp": peers[way]},
                device_id_type=pl.DeviceIdType.MESH,
            ).start()

    @pl.loop(1, CHUNKS)
    def _(k):
        load_wd(k).wait()
        load(CHUNKS + AHEAD + k)
        term = jnp.dot(hid_ref[0], wd_ref[k], preferred_element_type=jnp.float32)
        for way in (0, 1):
            at = (pl.ds(rows_of(n, block, me, way, 0), half), cols_of(k))
            y_ref[at] = term[way * half : (way + 1) * half].astype(y_ref.dtype)
            remote(way, 0, k).start()

    for copy in load_x(1):
        copy.wait()

    @pl.loop(0, CHUNKS)
    def _(j):
        hidden(1, j)

    @pl.loop(1, n)
    def _(step):
        slot = lax.rem(step, 2)
        more = step < n - 1

        @pl.when(more)
        def _():
            for copy in load_x(step + 1):
                copy.start()

        @pl.loop(0, CHUNKS)
        def _(k):
            term = jnp.dot(hid_ref[slot], wd_ref[k], preferred_element_type=jnp.float32)
            for way in (0, 1):
                arrive(way, step - 1, k)

            @pl.when(step > 1)
            def _():
                for way in (0, 1):
                    remote(way, step - 2, k).wait_send()

            for way in (0, 1):
                at = (pl.ds(rows_of(n, block, me, way, step), half), cols_of(k))
                total = y_ref[at].astype(jnp.float32) + term[way * half : (way + 1) * half]
                y_ref[at] = total.astype(y_ref.dtype)
                remote(way, step, k).start()

            @pl.when(jnp.logical_and(more, k == 0))
            def _():
                for copy in load_x(step + 1):
                    copy.wait()

            @pl.when(more)
            def _():
                hidden(1 - slot, k)

    cut, _ = split(n)

    @pl.loop(n * CHUNKS, cut)
    def _(i):
        step, k = i // CHUNKS, lax.rem(i, CHUNKS)
        for way in (0, 1):
            arrive(way, step - 1, k)
            remote(way, step - 2, k).wait_send()
            remote(way, step, k).start()

    @pl.loop(cut - CHUNKS, cut)
    def _(i):
        for way in (0, 1):
            arrive(way, i // CHUNKS, lax.rem(i, CHUNKS))

    @pl.loop(cut - 2 * CHUNKS, cut)
    def _(i):
        for way in (0, 1):
            remote(way, i // CHUNKS, lax.rem(i, CHUNKS)).wait_send()


def finish(n, y_ref, early_ref, late_ref, send_sem, recv_sem):
    del early_ref
    me = lax.axis_index("tp")
    peers = (lax.rem(me + 1, n), lax.rem(me + n - 1, n))
    block = y_ref.shape[0] // n
    half = block // 2
    cols = y_ref.shape[1] // CHUNKS
    cut, total = split(n)

    barrier = pltpu.get_barrier_semaphore()
    for peer in peers:
        pl.semaphore_signal(barrier, inc=1, device_id={"tp": peer}, device_id_type=pl.DeviceIdType.MESH)
    pl.semaphore_wait(barrier, 2)

    def remote(way, i, stored):
        at = pl.ds(pl.multiple_of(lax.rem(i, CHUNKS) * cols, 128), cols)
        rows = pl.ds(rows_of(n, block, me, way, i // CHUNKS), half)
        return pltpu.make_async_remote_copy(
            src_ref=late_ref.at[way, i - CHUNKS - cut] if stored else y_ref.at[rows, at],
            dst_ref=late_ref.at[way, i - cut],
            send_sem=send_sem.at[way, i - cut],
            recv_sem=recv_sem.at[way, i - cut],
            device_id={"tp": peers[way]},
            device_id_type=pl.DeviceIdType.MESH,
        )

    middle = jnp.minimum(cut + CHUNKS, total)

    @pl.loop(cut, middle)
    def _(i):
        for way in (0, 1):
            remote(way, i, False).start()

    @pl.loop(middle, total)
    def _(i):
        for way in (0, 1):
            remote(way, i - CHUNKS, False).wait_recv()
            remote(way, i, True).start()

    @pl.loop(jnp.maximum(cut, total - CHUNKS), total)
    def _(i):
        for way in (0, 1):
            remote(way, i, False).wait_recv()

    @pl.loop(cut, total)
    def _(i):
        for way in (0, 1):
            remote(way, i, False).wait_send()


def store(y_ref, out_ref, sem):
    rows = y_ref.shape[0] // STORES
    copies = [
        pltpu.make_async_copy(y_ref.at[pl.ds(i * rows, rows)], out_ref.at[pl.ds(i * rows, rows)], sem.at[i])
        for i in range(STORES)
    ]
    for copy in copies:
        copy.start()
    for copy in copies:
        copy.wait()


def store_late(n, early_ref, late_ref, out_ref, sem):
    del early_ref
    me = lax.axis_index("tp")
    block = out_ref.shape[0] // n
    cols = out_ref.shape[1] // CHUNKS
    cut, total = split(n)

    def copy(way, i):
        at = pl.ds(pl.multiple_of(lax.rem(i, CHUNKS) * cols, 128), cols)
        rows = pl.ds(rows_of(n, block, me, way, i // CHUNKS + 1), block // 2)
        return pltpu.make_async_copy(late_ref.at[way, i - cut], out_ref.at[rows, at], sem.at[way, i - cut])

    @pl.loop(cut, total)
    def _(i):
        for way in (0, 1):
            copy(way, i).start()

    @pl.loop(cut, total)
    def _(i):
        for way in (0, 1):
            copy(way, i).wait()


def solution(mesh):
    n = mesh.shape["tp"]
    hops = 2 * n - 2

    def step(x, w_gate, w_up, w_down):
        rows, width = x.shape
        units = w_gate.shape[1]
        block = rows // n
        y = pl.pallas_call(
            functools.partial(kernel, n),
            out_shape=pltpu.VMEM((rows, width), jnp.bfloat16),
            in_specs=[pl.BlockSpec(memory_space=pl.ANY)] * 4,
            out_specs=pl.BlockSpec(memory_space=pltpu.VMEM),
            scratch_shapes=[
                pltpu.VMEM((CHUNKS, width, 2 * units // CHUNKS), jnp.bfloat16),
                pltpu.VMEM((CHUNKS, units, width // CHUNKS), jnp.bfloat16),
                pltpu.VMEM((block, width), jnp.bfloat16),
                pltpu.VMEM((2, block, units), jnp.bfloat16),
                pltpu.SemaphoreType.DMA((2,)),
                pltpu.SemaphoreType.DMA((2, CHUNKS)),
                pltpu.SemaphoreType.DMA((CHUNKS,)),
                pltpu.SemaphoreType.DMA((2, hops, CHUNKS)),
                pltpu.SemaphoreType.DMA((2, hops, CHUNKS)),
            ],
            compiler_params=pltpu.CompilerParams(
                collective_id=0,
                has_side_effects=True,
                vmem_limit_bytes=VMEM_LIMIT - rows * width * 2,
            ),
        )(x, w_gate, w_up, w_down)
        y = pltpu.with_memory_space_constraint(y, pltpu.VMEM)
        anywhere = pl.BlockSpec(memory_space=pl.ANY)
        early = pl.pallas_call(
            store,
            out_shape=jax.ShapeDtypeStruct((rows, width), jnp.bfloat16),
            in_specs=[anywhere],
            out_specs=anywhere,
            scratch_shapes=[pltpu.SemaphoreType.DMA((STORES,))],
            compiler_params=pltpu.CompilerParams(vmem_limit_bytes=1 << 20),
        )(y)
        late = pl.pallas_call(
            functools.partial(finish, n),
            out_shape=pltpu.VMEM((2, LEFT[0], block // 2, width // CHUNKS), jnp.bfloat16),
            in_specs=[anywhere] * 2,
            out_specs=anywhere,
            scratch_shapes=[
                pltpu.SemaphoreType.DMA((2, LEFT[0])),
                pltpu.SemaphoreType.DMA((2, LEFT[0])),
            ],
            compiler_params=pltpu.CompilerParams(
                collective_id=1, has_side_effects=True, vmem_limit_bytes=1 << 20
            ),
        )(y, pltpu.with_memory_space_constraint(early, pltpu.HBM))
        late = pltpu.with_memory_space_constraint(late, pltpu.VMEM)
        return pl.pallas_call(
            functools.partial(store_late, n),
            out_shape=jax.ShapeDtypeStruct((rows, width), jnp.bfloat16),
            in_specs=[anywhere] * 2,
            out_specs=anywhere,
            input_output_aliases={0: 0},
            scratch_shapes=[pltpu.SemaphoreType.DMA((2, LEFT[0]))],
            compiler_params=pltpu.CompilerParams(vmem_limit_bytes=1 << 20),
        )(early, late)

    return jax.shard_map(
        step,
        mesh=mesh,
        in_specs=(P("dp", None), P(None, "tp"), P(None, "tp"), P("tp", None)),
        out_specs=P("dp", None),
        check_vma=False,
    )
```
